32 devices in a mesh: dp: 1 (over z), tp: 4 (over y), ep: 8 (over x, core).
Axes of the slice: x: 4, y: 4, z: 1, core: 2. Of those that a mesh axis runs over, the one named last changes fastest.
The devices are a block of a 4x4x8 slice.
Arguments:
- tokens: bfloat16 [8192, 2048], P(('dp', 'ep'))
- expert_ids: int32 [8192, 8], P(('dp', 'ep'))
- norm_gain: bfloat16 [2048], replicated
- router_w: bfloat16 [2048, 64], replicated
- w_gate: bfloat16 [64, 2048, 1024], P('ep', None, 'tp')
- w_up: bfloat16 [64, 2048, 1024], P('ep', None, 'tp')
- w_down: bfloat16 [64, 1024, 2048], P('ep', 'tp')
Outputs:
- output: bfloat16 [8192, 2048], P(('dp', 'ep'))
All inputs are finite; a program needn't handle non-finite values.
Results may differ from the reference program's by a relative error of at most 0.0119738.
Values are sent between devices in bfloat16 or wider.
A program may use at most 768 MiB of HBM per device.

```python
import jax
import jax.numpy as jnp
from jax import lax

MODEL_DIM = 2048
FFN_DIM = 1024
NUM_EXPERTS = 64
TOP_K = 8
EP_SIZE = 8
TOK_DEV = 1024
TOKENS = EP_SIZE * TOK_DEV
SLOT_CAP = 2 * TOP_K * TOK_DEV // NUM_EXPERTS
EXPERT_CAP = EP_SIZE * SLOT_CAP
NORM_EPS = 1e-5


def route_block(key):
    mean_load = TOP_K * TOK_DEV // NUM_EXPERTS
    key_lift, key_perm, key_tok = jax.random.split(key, 3)
    lifts = jax.random.randint(key_lift, (NUM_EXPERTS,), 1, mean_load, jnp.int32)
    lifts = lifts.at[0].set(mean_load).at[1].set(0)
    loads = mean_load + lifts - jnp.roll(lifts, -1)
    order = jnp.repeat(jnp.arange(NUM_EXPERTS, dtype=jnp.int32), loads, total_repeat_length=TOP_K * TOK_DEV)
    choice = order.reshape(TOP_K, TOK_DEV).T
    relabel = jax.random.permutation(key_perm, NUM_EXPERTS).astype(jnp.int32)
    shuffle = jax.random.permutation(key_tok, TOK_DEV)
    return relabel[choice][shuffle]


def setup_inputs(seed: int = 0, part: int = 0) -> dict:
    keys = jax.random.split(jax.random.key(seed), 5)
    tok_key = jax.random.fold_in(jax.random.key(seed + 1), part)
    route_key = jax.random.fold_in(jax.random.key(seed + 2), part)
    tokens = jax.random.normal(tok_key, (TOKENS, MODEL_DIM), jnp.float32)
    expert_ids = jax.vmap(route_block)(jax.random.split(route_key, EP_SIZE)).reshape(TOKENS, TOP_K)
    norm_gain = 1.0 + 0.5 * jax.random.normal(keys[0], (MODEL_DIM,), jnp.float32)
    router_w = jax.random.normal(keys[1], (MODEL_DIM, NUM_EXPERTS), jnp.float32) * MODEL_DIM ** -0.5
    w_gate = jax.random.normal(keys[2], (NUM_EXPERTS, MODEL_DIM, FFN_DIM), jnp.float32) * MODEL_DIM ** -0.5
    w_up = jax.random.normal(keys[3], (NUM_EXPERTS, MODEL_DIM, FFN_DIM), jnp.float32) * MODEL_DIM ** -0.5
    w_down = jax.random.normal(keys[4], (NUM_EXPERTS, FFN_DIM, MODEL_DIM), jnp.float32) * (2.0 * FFN_DIM ** -0.5)
    return {'tokens': tokens.astype(jnp.bfloat16), 'expert_ids': expert_ids, 'norm_gain': norm_gain.astype(jnp.bfloat16), 'router_w': router_w.astype(jnp.bfloat16), 'w_gate': w_gate.astype(jnp.bfloat16), 'w_up': w_up.astype(jnp.bfloat16), 'w_down': w_down.astype(jnp.bfloat16)}


def expert_ffn(operands):
    rows, gate_mat, up_mat, down_mat = operands
    gate_act = jnp.dot(rows, gate_mat, preferred_element_type=jnp.float32)
    up_act = jnp.dot(rows, up_mat, preferred_element_type=jnp.float32)
    hidden = (jax.nn.silu(gate_act) * up_act).astype(jnp.bfloat16)
    return jnp.dot(hidden, down_mat, preferred_element_type=jnp.float32).astype(jnp.bfloat16)


def reference(tokens, expert_ids, norm_gain, router_w, w_gate, w_up, w_down):
    tok_f32 = tokens.astype(jnp.float32)
    inv_rms = lax.rsqrt(jnp.mean(tok_f32 * tok_f32, axis=-1, keepdims=True) + NORM_EPS)
    normed = (tok_f32 * inv_rms * norm_gain.astype(jnp.float32)).astype(jnp.bfloat16)
    logits = jnp.dot(normed, router_w, preferred_element_type=jnp.float32)
    gates = jax.nn.softmax(jnp.take_along_axis(logits, expert_ids, axis=1), axis=-1)
    flat_ids = expert_ids.reshape(-1)
    onehot = (flat_ids[:, None] == jnp.arange(NUM_EXPERTS, dtype=jnp.int32)[None, :]).astype(jnp.int32)
    slot_ids = jnp.sum(jnp.cumsum(onehot, axis=0) * onehot, axis=1) - 1
    row_tok = jnp.arange(TOKENS * TOP_K, dtype=jnp.int32) // TOP_K
    src_rows = jnp.zeros((NUM_EXPERTS, EXPERT_CAP), jnp.int32).at[flat_ids, slot_ids].set(row_tok)
    buffers = normed[src_rows]
    expert_out = lax.map(expert_ffn, (buffers, w_gate, w_up, w_down))
    picked = expert_out[flat_ids, slot_ids].reshape(TOKENS, TOP_K, MODEL_DIM).astype(jnp.float32)
    mixed = jnp.sum(gates[:, :, None] * picked, axis=1)
    return (tok_f32 + mixed).astype(jnp.bfloat16)
```

```python
import functools

import jax
import jax.numpy as jnp
from jax import lax
from jax.experimental import pallas as pl
from jax.experimental.pallas import tpu as pltpu
from jax.sharding import PartitionSpec as P

NORM_EPS = 1e-5
NUM_CHUNKS = 2
ROW_TILE = 512
COL_TILE = 256


def route_dense(tokens, expert_ids, norm_gain, router_w):
    num_exp = router_w.shape[1]
    tok_f32 = tokens.astype(jnp.float32)
    inv_rms = lax.rsqrt(jnp.mean(tok_f32 * tok_f32, axis=-1, keepdims=True) + NORM_EPS)
    normed = (tok_f32 * inv_rms * norm_gain.astype(jnp.float32)).astype(jnp.bfloat16)
    logits = lax.dot_general(router_w, normed, (((0,), (1,)), ((), ())), preferred_element_type=jnp.float32)
    experts = jnp.arange(num_exp, dtype=jnp.int32)[:, None]
    ids = expert_ids.T
    chosen = functools.reduce(jnp.logical_or, [ids[k][None, :] == experts for k in range(ids.shape[0])])
    peak = jnp.max(jnp.where(chosen, logits, -jnp.inf), axis=0, keepdims=True)
    weight = jnp.where(chosen, jnp.exp(logits - peak), 0.0)
    return normed, weight / jnp.sum(weight, axis=0, keepdims=True)


def ffn_kernel(rows_ref, gate_ref, w1_ref, w3_ref, w2_ref, out_ref, hidden_ref, wide_ref):
    num_exp, width = w1_ref.shape[0], w1_ref.shape[2]
    tile = rows_ref.shape[0]
    for e in range(num_exp):
        wide_ref[e] = jnp.broadcast_to(gate_ref[:, e:e + 1], (tile, 128))

    def up(e, carry):
        rows = rows_ref[...]
        a = jnp.dot(rows, w1_ref[e], preferred_element_type=jnp.float32)
        b = jnp.dot(rows, w3_ref[e], preferred_element_type=jnp.float32)
        u = a * jax.nn.sigmoid(a) * b
        keep = jnp.concatenate([wide_ref[e]] * (width // 128), axis=1) > 0.0
        hidden_ref[e] = jnp.where(keep, u, 0.0).astype(jnp.bfloat16)
        return carry

    lax.fori_loop(0, num_exp, up, 0)

    def down(n, carry):
        cols = pl.ds(pl.multiple_of(n * COL_TILE, COL_TILE), COL_TILE)
        total = None
        for e in range(num_exp):
            y = jnp.dot(hidden_ref[e], w2_ref[e, :, cols], preferred_element_type=jnp.float32)
            term = jnp.concatenate([wide_ref[e]] * (COL_TILE // 128), axis=1) * y
            total = term if total is None else total + term
        out_ref[:, cols] = total
        return carry

    lax.fori_loop(0, out_ref.shape[1] // COL_TILE, down, 0)


def dense_experts(rows, gates, w_gate, w_up, w_down):
    num_rows, dim = rows.shape
    num_exp, _, width = w_gate.shape
    tile = min(ROW_TILE, num_rows)
    whole = lambda shape: pl.BlockSpec(shape, lambda i: (0,) * len(shape), pipeline_mode=pl.Buffered(1))
    return pl.pallas_call(
        ffn_kernel,
        out_shape=jax.ShapeDtypeStruct((num_rows, dim), jnp.float32),
        grid=(num_rows // tile,),
        in_specs=[pl.BlockSpec((tile, dim), lambda i: (i, 0)), pl.BlockSpec((tile, num_exp), lambda i: (i, 0)),
                  whole(w_gate.shape), whole(w_up.shape), whole(w_down.shape)],
        out_specs=pl.BlockSpec((tile, dim), lambda i: (i, 0)),
        scratch_shapes=[pltpu.VMEM((num_exp, tile, width), jnp.bfloat16), pltpu.VMEM((num_exp, tile, 128), jnp.float32)],
        compiler_params=pltpu.CompilerParams(dimension_semantics=("arbitrary",), vmem_limit_bytes=60 * 2**20),
        cost_estimate=pl.CostEstimate(flops=6 * num_rows * num_exp * dim * width, transcendentals=num_rows * num_exp * width,
                                      bytes_accessed=6 * num_rows * dim + 6 * num_exp * dim * width),
    )(rows, gates, w_gate, w_up, w_down)


def solution(mesh):
    ep_size, tp_size = mesh.shape['ep'], mesh.shape['tp']
    tok_spec = P(('dp', 'ep'), None)

    def local_block(tokens, expert_ids, norm_gain, router_w, w_gate, w_up, w_down):
        num_tok, dim = tokens.shape
        local_exp = w_gate.shape[0]
        normed, gates = route_dense(tokens, expert_ids, norm_gain, router_w)
        gates = lax.all_to_all(gates.reshape(ep_size, local_exp, num_tok), 'ep', 0, 0, tiled=True)
        gates = jnp.transpose(gates, (0, 2, 1))
        own_rows = num_tok // tp_size
        piece = own_rows // NUM_CHUNKS
        own_start = lax.axis_index('tp') * own_rows
        own_normed = lax.dynamic_slice_in_dim(normed, own_start, own_rows, 0)
        gates = gates.reshape(ep_size * tp_size, NUM_CHUNKS, piece, local_exp)
        mixed = []
        for c in range(NUM_CHUNKS):
            rows = lax.all_gather(own_normed[c * piece:(c + 1) * piece], ('ep', 'tp'), tiled=True)
            partial = dense_experts(rows, gates[:, c].reshape(rows.shape[0], local_exp), w_gate, w_up, w_down)
            mixed.append(lax.psum_scatter(partial, ('ep', 'tp'), scatter_dimension=0, tiled=True))
        own = lax.dynamic_slice_in_dim(tokens, own_start, own_rows, 0)
        done = (own.astype(jnp.float32) + jnp.concatenate(mixed, axis=0)).astype(jnp.bfloat16)
        return lax.all_gather(done, 'tp', tiled=True)

    return jax.shard_map(local_block, mesh=mesh, in_specs=(tok_spec, tok_spec, P(None), P(None, None), P('ep', None, 'tp'), P('ep', None, 'tp'), P('ep', 'tp', None)), out_specs=tok_spec, check_vma=False)
```

```python
import functools

import jax
import jax.numpy as jnp
from jax import lax
from jax.experimental import pallas as pl
from jax.experimental.pallas import tpu as pltpu
from jax.sharding import PartitionSpec as P

NORM_EPS = 1e-5
COL_TILE = 256
PIECE = 16
RING = 4


def route_dense(tokens, expert_ids, norm_gain, router_w):
    num_exp = router_w.shape[1]
    tok_f32 = tokens.astype(jnp.float32)
    inv_rms = lax.rsqrt(jnp.mean(tok_f32 * tok_f32, axis=-1, keepdims=True) + NORM_EPS)
    normed = (tok_f32 * inv_rms * norm_gain.astype(jnp.float32)).astype(jnp.bfloat16)
    logits = lax.dot_general(router_w, normed, (((0,), (1,)), ((), ())), preferred_element_type=jnp.float32)
    experts = jnp.arange(num_exp, dtype=jnp.int32)[:, None]
    ids = expert_ids.T
    chosen = functools.reduce(jnp.logical_or, [ids[k][None, :] == experts for k in range(ids.shape[0])])
    peak = jnp.max(jnp.where(chosen, logits, -jnp.inf), axis=0, keepdims=True)
    weight = jnp.where(chosen, jnp.exp(logits - peak), 0.0)
    return normed, weight / jnp.sum(weight, axis=0, keepdims=True)


def moe_kernel(steps, keep, h_ref, tok_ref, gate_ref, w1_ref, w3_ref, w2_ref, out_ref, pool_ref,
               rows_buf, gate_buf, hidden_ref, wide_ref, mine, other, part, from_far, from_front, from_back, quarter, from_x,
               own_sem, own_front_send, own_back_send, relay_send, pair_send, back_recv, front_recv, far_recv, pair_recv,
               load_sem, sum_send, sum_recv, far_send, far_sum_recv, near_send, near_recv, relay_sum_send, relay_sum_recv, x_send, x_recv):
    num_exp, width = w1_ref.shape[0], w1_ref.shape[2]
    dim = h_ref.shape[2]
    ep, y = lax.axis_index("ep"), lax.axis_index("tp")
    x, core = ep // 2, ep % 2
    turn = 1 + 2 * core
    xf, xb, yf, yb = (x + turn) % RING, (x + RING - turn) % RING, (y + turn) % RING, (y + RING - turn) % RING
    xo, yo = (x + 2) % RING, (y + 2) % RING
    at_x = lambda other_x: {"ep": other_x * 2 + core}
    at_y = lambda other_y: {"tp": other_y}
    pair = {"ep": x * 2 + 1 - core}

    def remote(src, dst, send, recv, to):
        return pltpu.make_async_remote_copy(src_ref=src, dst_ref=dst, send_sem=send, recv_sem=recv, device_id=to, device_id_type=pl.DeviceIdType.MESH)

    barrier = pltpu.get_barrier_semaphore()
    peers = (pair, at_x(xf), at_x(xb), at_x(xo), at_y(yf), at_y(yb))
    for peer in peers:
        pl.semaphore_signal(barrier, inc=1, device_id=peer, device_id_type=pl.DeviceIdType.MESH)
    pl.semaphore_wait(barrier, len(peers))

    def within(chunk):
        return jnp.logical_and(chunk >= 0, chunk < steps)

    own_copy = lambda k: pltpu.make_async_copy(h_ref.at[k], pool_ref.at[k, core, x], own_sem.at[k])
    own_front = lambda k: remote(h_ref.at[k], pool_ref.at[k, core, x], own_front_send.at[k], back_recv.at[k], at_x(xf))
    own_back = lambda k: remote(h_ref.at[k], pool_ref.at[k, core, x], own_back_send.at[k], front_recv.at[k], at_x(xb))
    relay = lambda k: remote(pool_ref.at[k, core, xb], pool_ref.at[k, core, xb], relay_send.at[k], far_recv.at[k], at_x(xf))
    to_pair = lambda k: remote(pool_ref.at[k, core], pool_ref.at[k, core], pair_send.at[k], pair_recv.at[k], pair)

    def loads(k, slot):
        return [pltpu.make_async_copy(pool_ref.at[k, core], rows_buf.at[slot, 0], load_sem.at[slot, 0]),
                pltpu.make_async_copy(pool_ref.at[k, 1 - core], rows_buf.at[slot, 1], load_sem.at[slot, 1]),
                pltpu.make_async_copy(gate_ref.at[k, core], gate_buf.at[slot, 0], load_sem.at[slot, 2]),
                pltpu.make_async_copy(gate_ref.at[k, 1 - core], gate_buf.at[slot, 1], load_sem.at[slot, 3])]

    sum_copy = lambda k: remote(other, part.at[k % keep], sum_send, sum_recv.at[k % keep], pair)
    far_copy = lambda k: remote(part.at[k % keep, :, yo], from_far.at[k % keep], far_send, far_sum_recv.at[k % keep], at_y(yf))
    near_copy = lambda k: remote(part.at[k % keep, :, yb], from_front.at[k % keep], near_send, near_recv.at[k % keep], at_y(yb))
    next_copy = lambda k: remote(part.at[k % keep, :, yf], from_back.at[k % keep], relay_sum_send, relay_sum_recv.at[k % keep], at_y(yf))
    x_copies = lambda k: [remote(quarter.at[k % 2, (x + d) % RING], from_x.at[k % keep, d - 1], x_send.at[d - 1], x_recv.at[k % keep, d - 1],
                                 at_x((x + d) % RING)) for d in range(1, RING)]

    def gather_ahead(t):
        @pl.when(within(t + 4))
        def _():
            own_copy(t + 4).start()
            own_front(t + 4).start()
            own_back(t + 4).start()

        @pl.when(within(t + 3))
        def _():
            own_front(t + 3).wait_recv()
            relay(t + 3).start()

        @pl.when(within(t + 2))
        def _():
            own_back(t + 2).wait_recv()
            relay(t + 2).wait_recv()
            own_copy(t + 2).wait()
            to_pair(t + 2).start()

        @pl.when(within(t + 1))
        def _():
            to_pair(t + 1).wait_recv()
            for copy in loads(t + 1, (t + 1) % 2):
                copy.start()

    def experts(t):
        slot = t % 2
        for copy in loads(t, slot):
            copy.wait()
        half = wide_ref.shape[1] // 2
        for e in range(num_exp):
            for p in range(2):
                wide_ref[e, p * half:(p + 1) * half] = jnp.broadcast_to(gate_buf[slot, p, :, e:e + 1], (half, 128))

        def up(e, carry):
            rows = rows_buf[slot].reshape(2 * half, dim)
            a = jnp.dot(rows, w1_ref[e], preferred_element_type=jnp.float32)
            b = jnp.dot(rows, w3_ref[e], preferred_element_type=jnp.float32)
            u = a * jax.nn.sigmoid(a) * b
            chosen = jnp.concatenate([wide_ref[e]] * (width // 128), axis=1) > 0.0
            hidden_ref[e] = jnp.where(chosen, u, 0.0).astype(jnp.bfloat16)
            return carry

        lax.fori_loop(0, num_exp, up, 0)

        @pl.when(t >= 1)
        def _():
            sum_copy(t - 1).wait_send()

        def down(n, carry):
            cols = pl.ds(pl.multiple_of(n * COL_TILE, COL_TILE), COL_TILE)
            total = None
            for e in range(num_exp):
                term = jnp.concatenate([wide_ref[e]] * (COL_TILE // 128), axis=1) * jnp.dot(hidden_ref[e], w2_ref[e, :, cols], preferred_element_type=jnp.float32)
                total = term if total is None else total + term
            total = total.reshape((2,) + other.shape[:3] + (COL_TILE,))
            mine[slot, :, :, :, cols] = total[0]
            other[:, :, :, cols] = total[1]
            return carry

        lax.fori_loop(0, dim // COL_TILE, down, 0)

    def reduce_behind(t):
        @pl.when(within(t - 2))
        def _():
            far_copy(t - 2).wait_send()
            near_copy(t - 2).wait_send()

        @pl.when(within(t - 3))
        def _():
            next_copy(t - 3).wait_send()

        @pl.when(within(t - 4))
        def _():
            k = t - 4
            for copy in x_copies(k):
                copy.wait_send()
            for copy in x_copies(k):
                copy.wait_recv()
            mixed = quarter[k % 2, x] + from_x[k % keep, 0] + from_x[k % keep, 1] + from_x[k % keep, 2]
            out_ref[k] = (tok_ref[k].astype(jnp.float32) + mixed).astype(jnp.bfloat16)

        @pl.when(within(t - 3))
        def _():
            k = t - 3
            near_copy(k).wait_recv()
            next_copy(k).wait_recv()
            for i in range(RING):
                quarter[k % 2, i] = part[k % keep, i, y] + from_front[k % keep, i] + from_back[k % keep, i]
            for copy in x_copies(k):
                copy.start()

        @pl.when(within(t - 2))
        def _():
            k = t - 2
            far_copy(k).wait_recv()
            for i in range(RING):
                part[k % keep, i, yf] = part[k % keep, i, yf] + from_far[k % keep, i]
            next_copy(k).start()

        @pl.when(within(t - 1))
        def _():
            k = t - 1
            sum_copy(k).wait_recv()

            def add(i, carry):
                for q in range(RING):
                    part[k % keep, i, q] = part[k % keep, i, q] + mine[k % 2, i, q]
                return carry

            lax.fori_loop(0, RING, add, 0)
            far_copy(k).start()
            near_copy(k).start()

        @pl.when(within(t))
        def _():
            sum_copy(t).start()

    def step(i, carry):
        t = i - 4
        gather_ahead(t)
        pl.when(within(t))(lambda: experts(t))
        reduce_behind(t)
        return carry

    lax.fori_loop(0, steps + 8, step, 0)
    sum_copy(steps - 1).wait_send()

    def drain(k, carry):
        own_front(k).wait_send()
        own_back(k).wait_send()
        relay(k).wait_send()
        to_pair(k).wait_send()
        return carry

    lax.fori_loop(0, steps, drain, 0)


def fused_experts(h, tok, gates, w_gate, w_up, w_down):
    steps, rows, dim = h.shape
    num_exp, _, width = w_gate.shape
    piece, keep = rows // RING, 4
    chunk = 2 * RING * rows
    vmem = pl.BlockSpec(memory_space=pltpu.VMEM)
    hbm = pl.BlockSpec(memory_space=pl.ANY)
    quad = (RING, RING, piece, dim)
    dma = pltpu.SemaphoreType.DMA
    out, _ = pl.pallas_call(
        functools.partial(moe_kernel, steps, keep),
        out_shape=(jax.ShapeDtypeStruct((steps, piece, dim), jnp.bfloat16), jax.ShapeDtypeStruct((steps, 2, RING, rows, dim), jnp.bfloat16)),
        in_specs=[hbm, vmem, hbm, vmem, vmem, vmem],
        out_specs=(vmem, hbm),
        scratch_shapes=[
            pltpu.VMEM((2, 2, RING, rows, dim), jnp.bfloat16), pltpu.VMEM((2, 2, chunk // 2, num_exp), jnp.float32),
            pltpu.VMEM((num_exp, chunk, width), jnp.bfloat16), pltpu.VMEM((num_exp, chunk, 128), jnp.float32),
            pltpu.VMEM((2,) + quad, jnp.float32), pltpu.VMEM(quad, jnp.float32), pltpu.VMEM((keep,) + quad, jnp.float32),
            pltpu.VMEM((keep, RING, piece, dim), jnp.float32), pltpu.VMEM((keep, RING, piece, dim), jnp.float32),
            pltpu.VMEM((keep, RING, piece, dim), jnp.float32), pltpu.VMEM((2, RING, piece, dim), jnp.float32),
            pltpu.VMEM((keep, RING - 1, piece, dim), jnp.float32),
            dma((steps,)), dma((steps,)), dma((steps,)), dma((steps,)), dma((steps,)), dma((steps,)), dma((steps,)), dma((steps,)), dma((steps,)),
            dma((2, 4)), dma, dma((keep,)), dma, dma((keep,)), dma, dma((keep,)), dma, dma((keep,)), dma((RING - 1,)), dma((keep, RING - 1)),
        ],
        compiler_params=pltpu.CompilerParams(collective_id=0, has_side_effects=True, vmem_limit_bytes=67043328),
        cost_estimate=pl.CostEstimate(flops=6 * steps * chunk * num_exp * dim * width, transcendentals=steps * chunk * num_exp * width,
                                      bytes_accessed=2 * steps * chunk * dim + 6 * num_exp * dim * width),
    )(h, tok, gates, w_gate, w_up, w_down)
    return out


def solution(mesh):
    ep_size, tp_size = mesh.shape['ep'], mesh.shape['tp']
    tok_spec = P(('dp', 'ep'), None)

    def local_block(tokens, expert_ids, norm_gain, router_w, w_gate, w_up, w_down):
        num_tok, dim = tokens.shape
        local_exp = w_gate.shape[0]
        normed, gates = route_dense(tokens, expert_ids, norm_gain, router_w)
        own_rows = num_tok // tp_size
        steps = own_rows // PIECE
        gates = lax.all_to_all(gates.reshape(ep_size, local_exp, num_tok), 'ep', 0, 0, tiled=True)
        gates = gates.reshape(ep_size // 2, 2, local_exp, tp_size, steps, PIECE)
        gates = jnp.transpose(gates, (4, 1, 0, 3, 5, 2)).reshape(steps, 2, ep_size // 2 * tp_size * PIECE, local_exp)
        h = jnp.transpose(normed.reshape(tp_size, steps, PIECE, dim), (1, 0, 2, 3)).reshape(steps, tp_size * PIECE, dim)
        own = lax.dynamic_slice_in_dim(tokens, lax.axis_index('tp') * own_rows, own_rows, 0).reshape(steps, PIECE, dim)
        done = fused_experts(h, own, gates, w_gate, w_up, w_down)
        return lax.all_gather(done.reshape(own_rows, dim), 'tp', tiled=True)

    return jax.shard_map(local_block, mesh=mesh, in_specs=(tok_spec, tok_spec, P(None), P(None, None), P('ep', None, 'tp'), P('ep', None, 'tp'), P('ep', 'tp', None)), out_specs=tok_spec, check_vma=False)
```

```python
import functools

import jax
import jax.numpy as jnp
from jax import lax
from jax.experimental import pallas as pl
from jax.experimental.pallas import tpu as pltpu
from jax.sharding import PartitionSpec as P

NORM_EPS = 1e-5
COL_TILE = 256
PIECE = 16
RING = 4
KEEP = 5


def route_dense(tokens, expert_ids, norm_gain, router_w):
    num_exp = router_w.shape[1]
    tok_f32 = tokens.astype(jnp.float32)
    inv_rms = lax.rsqrt(jnp.mean(tok_f32 * tok_f32, axis=-1, keepdims=True) + NORM_EPS)
    normed = (tok_f32 * inv_rms * norm_gain.astype(jnp.float32)).astype(jnp.bfloat16)
    logits = lax.dot_general(router_w, normed, (((0,), (1,)), ((), ())), preferred_element_type=jnp.float32)
    experts = jnp.arange(num_exp, dtype=jnp.int32)[:, None]
    ids = expert_ids.T
    chosen = functools.reduce(jnp.logical_or, [ids[k][None, :] == experts for k in range(ids.shape[0])])
    peak = jnp.max(jnp.where(chosen, logits, -jnp.inf), axis=0, keepdims=True)
    weight = jnp.where(chosen, jnp.exp(logits - peak), 0.0)
    return normed, weight / jnp.sum(weight, axis=0, keepdims=True)


def moe_kernel(steps, keep, h_ref, tok_ref, gate_ref, w1_hbm, w3_hbm, w2_hbm, out_ref, pool_ref,
               w1_ref, w3_ref, w2_ref, out_buf, rows_buf, gate_buf, hidden_ref, wide_ref, mine, other, part, from_far, from_front, from_back, quarter, from_x,
               own_sem, own_front_send, own_back_send, relay_send, pair_send, back_recv, front_recv, far_recv, pair_recv,
               load_sem, sum_send, sum_recv, far_send, far_sum_recv, near_send, near_recv, relay_sum_send, relay_sum_recv, x_send, x_recv,
               weight_sem, out_sem, out_front_send, out_back_send, out_relay_send, out_back_recv, out_front_recv, out_far_recv):
    num_exp, width = w1_ref.shape[0], w1_ref.shape[2]
    dim = h_ref.shape[3]
    ep, y = lax.axis_index("ep"), lax.axis_index("tp")
    x, core = ep // 2, ep % 2
    turn = 1 + 2 * core
    xf, xb, yf, yb = (x + turn) % RING, (x + RING - turn) % RING, (y + turn) % RING, (y + RING - turn) % RING
    xo, yo = (x + 2) % RING, (y + 2) % RING
    at_x = lambda other_x: {"ep": other_x * 2 + core}
    at_y = lambda other_y: {"tp": other_y}
    pair = {"ep": x * 2 + 1 - core}

    def remote(src, dst, send, recv, to):
        return pltpu.make_async_remote_copy(src_ref=src, dst_ref=dst, send_sem=send, recv_sem=recv, device_id=to, device_id_type=pl.DeviceIdType.MESH)

    barrier = pltpu.get_barrier_semaphore()
    peers = (pair, at_x(xf), at_x(xb), at_x(xo), at_y(yf), at_y(yb))
    for peer in peers:
        pl.semaphore_signal(barrier, inc=1, device_id=peer, device_id_type=pl.DeviceIdType.MESH)
    pl.semaphore_wait(barrier, len(peers))

    def within(chunk):
        return jnp.logical_and(chunk >= 0, chunk < steps)

    own_copy = lambda k: pltpu.make_async_copy(h_ref.at[:, k], pool_ref.at[k, core, x], own_sem.at[k])
    own_front = lambda k: remote(h_ref.at[:, k], pool_ref.at[k, core, x], own_front_send.at[k], back_recv.at[k], at_x(xf))
    own_back = lambda k: remote(h_ref.at[:, k], pool_ref.at[k, core, x], own_back_send.at[k], front_recv.at[k], at_x(xb))
    relay = lambda k: remote(pool_ref.at[k, core, xb], pool_ref.at[k, core, xb], relay_send.at[k], far_recv.at[k], at_x(xf))
    to_pair = lambda k: remote(pool_ref.at[k, core], pool_ref.at[k, core], pair_send.at[k], pair_recv.at[k], pair)

    def loads(k, slot):
        return [pltpu.make_async_copy(pool_ref.at[k, core], rows_buf.at[slot, 0], load_sem.at[slot, 0]),
                pltpu.make_async_copy(pool_ref.at[k, 1 - core], rows_buf.at[slot, 1], load_sem.at[slot, 1]),
                pltpu.make_async_copy(gate_ref.at[k, core], gate_buf.at[slot, 0], load_sem.at[slot, 2]),
                pltpu.make_async_copy(gate_ref.at[k, 1 - core], gate_buf.at[slot, 1], load_sem.at[slot, 3])]

    weights = [pltpu.make_async_copy(src, dst, weight_sem.at[i]) for i, (src, dst) in enumerate(((w1_hbm, w1_ref), (w3_hbm, w3_ref), (w2_hbm, w2_ref)))]
    for copy in weights:
        copy.start()

    sum_copy = lambda k: remote(other, part.at[k % keep], sum_send, sum_recv.at[k % keep], pair)

    def reduce_copies(k):
        slot = k % keep
        far = remote(part.at[slot, :, yo], from_far.at[slot], far_send, far_sum_recv.at[slot], at_y(yf))
        near = remote(part.at[slot, :, yb], from_front.at[slot], near_send, near_recv.at[slot], at_y(yb))
        onward = remote(part.at[slot, :, yf], from_back.at[slot], relay_sum_send, relay_sum_recv.at[slot], at_y(yf))
        direct = [remote(quarter.at[k % 2, (x + d) % RING], from_x.at[slot, d - 1], x_send.at[d - 1], x_recv.at[slot, d - 1],
                         at_x((x + d) % RING)) for d in range(1, RING)]
        return far, near, onward, direct

    out_copy = lambda k: pltpu.make_async_copy(out_buf.at[k % 2], out_ref.at[y, k], out_sem.at[k % 2])
    out_front = lambda k: remote(out_buf.at[k % 2], out_ref.at[y, k], out_front_send.at[k % 2], out_back_recv.at[k], at_y(yf))
    out_back = lambda k: remote(out_buf.at[k % 2], out_ref.at[y, k], out_back_send.at[k % 2], out_front_recv.at[k], at_y(yb))
    out_relay = lambda k: remote(out_ref.at[yb, k], out_ref.at[yb, k], out_relay_send.at[k], out_far_recv.at[k], at_y(yf))

    def gather_ahead(t):
        @pl.when(within(t + 4))
        def _():
            own_copy(t + 4).start()
            own_front(t + 4).start()
            own_back(t + 4).start()

        @pl.when(within(t + 3))
        def _():
            own_front(t + 3).wait_recv()
            relay(t + 3).start()

        @pl.when(within(t + 2))
        def _():
            own_back(t + 2).wait_recv()
            relay(t + 2).wait_recv()
            own_copy(t + 2).wait()
            to_pair(t + 2).start()

        @pl.when(within(t + 1))
        def _():
            to_pair(t + 1).wait_recv()
            for copy in loads(t + 1, (t + 1) % 2):
                copy.start()

    def experts_up(t):
        slot = t % 2
        for copy in loads(t, slot):
            copy.wait()

        @pl.when(t == 0)
        def _():
            for copy in weights:
                copy.wait()

        half = wide_ref.shape[1] // 2
        for e in range(num_exp):
            for p in range(2):
                wide_ref[e, p * half:(p + 1) * half] = jnp.broadcast_to(gate_buf[slot, p, :, e:e + 1], (half, 128))

        def up(e, carry):
            rows = rows_buf[slot].reshape(2 * half, dim)
            a = jnp.dot(rows, w1_ref[e], preferred_element_type=jnp.float32)
            b = jnp.dot(rows, w3_ref[e], preferred_element_type=jnp.float32)
            u = a * jax.nn.sigmoid(a) * b
            chosen = jnp.concatenate([wide_ref[e]] * (width // 128), axis=1) > 0.0
            hidden_ref[e] = jnp.where(chosen, u, 0.0).astype(jnp.bfloat16)
            return carry

        lax.fori_loop(0, num_exp, up, 0, unroll=8)

    def experts_down(t):
        slot = t % 2

        @pl.when(t >= 1)
        def _():
            sum_copy(t - 1).wait_send()

        def down(n, carry):
            cols = pl.ds(pl.multiple_of(n * COL_TILE, COL_TILE), COL_TILE)
            total = None
            for e in range(num_exp):
                term = jnp.concatenate([wide_ref[e]] * (COL_TILE // 128), axis=1) * jnp.dot(hidden_ref[e], w2_ref[e, :, cols], preferred_element_type=jnp.float32)
                total = term if total is None else total + term
            total = total.reshape((2,) + other.shape[:3] + (COL_TILE,))
            mine[slot, :, :, :, cols] = total[0]
            other[:, :, :, cols] = total[1]
            return carry

        lax.fori_loop(0, dim // COL_TILE, down, 0, unroll=2)

    def if_within(chunk, body):
        pl.when(within(chunk))(lambda: body(chunk))

    def reduce_between(t):
        def sent_onward(k):
            reduce_copies(k)[2].wait_send()

        def pass_on(k):
            far, _, onward, _ = reduce_copies(k)
            far.wait_recv()
            for i in range(RING):
                part[k % keep, i, yf] = part[k % keep, i, yf] + from_far[k % keep, i]
            onward.start()

        if_within(t - 4, sent_onward)
        if_within(t - 3, pass_on)

    def reduce_behind(t):
        def sent_first(k):
            far, near, _, _ = reduce_copies(k)
            far.wait_send()
            near.wait_send()

        def finish(k):
            direct = reduce_copies(k)[3]
            for copy in direct:
                copy.wait_send()
            for copy in direct:
                copy.wait_recv()
            mixed = quarter[k % 2, x] + from_x[k % keep, 0] + from_x[k % keep, 1] + from_x[k % keep, 2]
            out_buf[k % 2] = (tok_ref[k].astype(jnp.float32) + mixed).astype(jnp.bfloat16)
            out_copy(k).start()
            out_front(k).start()
            out_back(k).start()

        def spread(k):
            _, near, onward, direct = reduce_copies(k)
            near.wait_recv()
            onward.wait_recv()
            for i in range(RING):
                quarter[k % 2, i] = part[k % keep, i, y] + from_front[k % keep, i] + from_back[k % keep, i]
            for copy in direct:
                copy.start()

        def begin(k):
            far, near, _, _ = reduce_copies(k)
            far.start()
            near.start()

        if_within(t - 2, sent_first)

        @pl.when(within(t - 7))
        def _():
            out_copy(t - 7).wait()
            out_front(t - 7).wait_send()
            out_back(t - 7).wait_send()

        @pl.when(within(t - 6))
        def _():
            out_front(t - 6).wait_recv()
            out_relay(t - 6).start()

        if_within(t - 5, finish)
        if_within(t - 4, spread)

        @pl.when(within(t - 1))
        def _():
            k = t - 1
            sum_copy(k).wait_recv()

            def add(i, carry):
                for q in range(RING):
                    part[k % keep, i, q] = part[k % keep, i, q] + mine[k % 2, i, q]
                return carry

            lax.fori_loop(0, RING, add, 0)

        if_within(t - 1, begin)

        @pl.when(within(t))
        def _():
            sum_copy(t).start()

    def step(i, carry):
        t = i - 4
        gather_ahead(t)
        pl.when(within(t))(lambda: experts_up(t))
        reduce_between(t)
        pl.when(within(t))(lambda: experts_down(t))
        reduce_behind(t)
        return carry

    lax.fori_loop(0, steps + 12, step, 0)
    sum_copy(steps - 1).wait_send()

    def drain(k, carry):
        own_front(k).wait_send()
        own_back(k).wait_send()
        relay(k).wait_send()
        to_pair(k).wait_send()
        out_relay(k).wait_send()
        out_back(k).wait_recv()
        out_relay(k).wait_recv()
        return carry

    lax.fori_loop(0, steps, drain, 0)


def fused_experts(h, tok, gates, w_gate, w_up, w_down):
    _, steps, piece, dim = h.shape
    num_exp, _, width = w_gate.shape
    keep = KEEP
    chunk = 2 * RING * RING * piece
    vmem = pl.BlockSpec(memory_space=pltpu.VMEM)
    hbm = pl.BlockSpec(memory_space=pl.ANY)
    quad = (RING, RING, piece, dim)
    dma = pltpu.SemaphoreType.DMA
    out, _ = pl.pallas_call(
        functools.partial(moe_kernel, steps, keep),
        out_shape=(jax.ShapeDtypeStruct((RING, steps, piece, dim), jnp.bfloat16), jax.ShapeDtypeStruct((steps, 2) + quad, jnp.bfloat16)),
        in_specs=[hbm, vmem, hbm, hbm, hbm, hbm],
        out_specs=(hbm, hbm),
        scratch_shapes=[
            pltpu.VMEM(w_gate.shape, w_gate.dtype), pltpu.VMEM(w_up.shape, w_up.dtype), pltpu.VMEM(w_down.shape, w_down.dtype),
            pltpu.VMEM((2, piece, dim), jnp.bfloat16),
            pltpu.VMEM((2, 2) + quad, jnp.bfloat16), pltpu.VMEM((2, 2, chunk // 2, num_exp), jnp.float32),
            pltpu.VMEM((num_exp, chunk, width), jnp.bfloat16), pltpu.VMEM((num_exp, chunk, 128), jnp.float32),
            pltpu.VMEM((2,) + quad, jnp.float32), pltpu.VMEM(quad, jnp.float32), pltpu.VMEM((keep,) + quad, jnp.float32),
            pltpu.VMEM((keep, RING, piece, dim), jnp.float32), pltpu.VMEM((keep, RING, piece, dim), jnp.float32),
            pltpu.VMEM((keep, RING, piece, dim), jnp.float32), pltpu.VMEM((2, RING, piece, dim), jnp.float32),
            pltpu.VMEM((keep, RING - 1, piece, dim), jnp.float32),
            dma((steps,)), dma((steps,)), dma((steps,)), dma((steps,)), dma((steps,)), dma((steps,)), dma((steps,)), dma((steps,)), dma((steps,)),
            dma((2, 4)), dma, dma((keep,)), dma, dma((keep,)), dma, dma((keep,)), dma, dma((keep,)), dma((RING - 1,)), dma((keep, RING - 1)),
            dma((3,)), dma((2,)), dma((2,)), dma((2,)), dma((steps,)), dma((steps,)), dma((steps,)), dma((steps,)),
        ],
        compiler_params=pltpu.CompilerParams(collective_id=0, has_side_effects=True, vmem_limit_bytes=67043328),
        cost_estimate=pl.CostEstimate(flops=6 * steps * chunk * num_exp * dim * width, transcendentals=steps * chunk * num_exp * width,
                                      bytes_accessed=2 * steps * chunk * dim + 6 * num_exp * dim * width),
    )(h, tok, gates, w_gate, w_up, w_down)
    return out


def solution(mesh):
    ep_size, tp_size = mesh.shape['ep'], mesh.shape['tp']
    tok_spec = P(('dp', 'ep'), None)

    def local_block(tokens, expert_ids, norm_gain, router_w, w_gate, w_up, w_down):
        num_tok, dim = tokens.shape
        local_exp = w_gate.shape[0]
        normed, gates = route_dense(tokens, expert_ids, norm_gain, router_w)
        own_rows = num_tok // tp_size
        steps = own_rows // PIECE
        gates = lax.all_to_all(gates.reshape(ep_size, local_exp, num_tok), 'ep', 0, 0, tiled=True)
        gates = gates.reshape(ep_size // 2, 2, local_exp, tp_size, steps, PIECE)
        gates = jnp.transpose(gates, (4, 1, 0, 3, 5, 2)).reshape(steps, 2, ep_size // 2 * tp_size * PIECE, local_exp)
        h = normed.reshape(tp_size, steps, PIECE, dim)
        own = lax.dynamic_slice_in_dim(tokens, lax.axis_index('tp') * own_rows, own_rows, 0).reshape(steps, PIECE, dim)
        done = fused_experts(h, own, gates, w_gate, w_up, w_down)
        return done.reshape(num_tok, dim)

    return jax.shard_map(local_block, mesh=mesh, in_specs=(tok_spec, tok_spec, P(None), P(None, None), P('ep', None, 'tp'), P('ep', None, 'tp'), P('ep', 'tp', None)), out_specs=tok_spec, check_vma=False)
```
